32 devices in a mesh: dom: 4 (over z), feat: 8 (over y, x, core).
Axes of the slice: x: 2, y: 2, z: 4, core: 2. Of those that a mesh axis runs over, the one named last changes fastest.
Arguments:
- node_feats: bfloat16 [4096, 512], P('dom', 'feat'), may hold values from -6 to 6
- rel_weight: bfloat16 [4, 512, 512], replicated, may hold values from -0.25 to 0.25
- self_weight: bfloat16 [512, 512], replicated, may hold values from -0.25 to 0.25
- bias: float32 [512], replicated, may hold values from -3 to 3
- out_degree: int32 [4, 4096], P(None, 'dom'), may hold values from 0 to 63
- adjacency: int32 [4, 8, 64, 256, 256], P('dom', 'feat'), may hold values 0 or 1
- tile_index: int32 [4, 8, 64, 3], P('dom', 'feat'), may hold values from 0 to 15, as said below
- tile_count: int32 [4, 8], P('dom', 'feat'), may hold values from 1 to 64, as said below
Outputs:
- embedding: bfloat16 [4096, 512], P('dom', 'feat')
The draws below stay inside these ranges and needn't reach their ends.
Inputs may be any that keep to these rules, and one draw needn't show every extreme that they name: `tile_index`: the three entries of a slot are a relation below 4, a destination block below 16 and a source block of the device's own group below 4; entries of slots beyond a device's count are arbitrary within the range. `tile_count`: some device holds exactly 64 live slots.
All inputs are finite; a program needn't handle non-finite values. No bound on the sum of `adjacency` on one device may be relied on, other than what follows from the above.
Results may differ from the reference program's by a relative error of at most 0.0049.
Values may be sent and summed in bfloat16 or wider, within the bound.
A program may use at most 128 MiB of HBM per device.

```python
import jax
import jax.numpy as jnp
from jax import lax

H = 512
R = 4
TILE_SIZE = 256
BG = 4
TILE_DEV = 64
NODES = 4096
N_DOM = 4
N_FEAT = 8


def draw_tile_index(key, part):
    first, second, third = jax.random.split(jax.random.fold_in(key, 11), 3)
    shape = (N_DOM, N_FEAT, TILE_DEV)
    relation = jax.random.randint(first, shape, 0, R)
    target = jax.random.randint(second, shape, 0, N_DOM * BG)
    source = jax.random.randint(third, shape, 0, BG)
    return jnp.stack([relation, target, source], axis=-1).astype(jnp.int32)


def draw_tile_count(key, part):
    first, second = jax.random.split(jax.random.fold_in(key, 23), 2)
    counts = jax.random.randint(first, (N_DOM * N_FEAT,), 1, TILE_DEV + 1)
    position = jax.random.randint(second, (), 0, N_DOM * N_FEAT)
    positions = jnp.arange(N_DOM * N_FEAT)
    counts = jnp.where(positions == position, TILE_DEV, counts)
    return counts.reshape(N_DOM, N_FEAT).astype(jnp.int32)


def touch_ends(result, stream_key, low, largest):
    spot = [jax.random.randint(jax.random.fold_in(stream_key, axis), (), 0, length) for axis, length in enumerate(result.shape)]
    longest = result.shape.index(max(result.shape))
    next_to = spot[:longest] + [(spot[longest] + 1) % result.shape[longest]] + spot[longest + 1:]
    return result.at[tuple(spot)].set(low).at[tuple(next_to)].set(largest)


def block_levels(stream_key, shape, cuts, low, largest):
    factor_of, own = 1.0, jax.random.fold_in(stream_key, 6)
    for axis_at, blocks in cuts:
        heights = jnp.exp(jax.random.uniform(jax.random.fold_in(own, axis_at), (blocks,), jnp.float32, low / len(cuts), largest / len(cuts)))
        factor_of = factor_of * jnp.repeat(heights, shape[axis_at] // blocks).reshape([-1 if axis == axis_at else 1 for axis in range(len(shape))])
    return factor_of


def noise(stream_key, extent, spread, reach, pieces=(), kind=jnp.bfloat16):
    array = spread * jax.random.normal(stream_key, extent, jnp.float32)
    if pieces:
        array = array * block_levels(stream_key, extent, pieces, -0.22, 0.18)
    return jnp.clip(array, -reach, reach).astype(kind)


def setup_inputs(seed: int = 0) -> dict:
    key_of = jax.random.split(jax.random.key(seed), 9)
    node_feats = noise(key_of[0], (NODES, H), 1.0, 6.0, ((0, 4), (1, 8)))
    rel_weight = noise(key_of[1], (R, H, H), H ** -0.5, 0.25)
    self_weight = noise(key_of[2], (H, H), H ** -0.5, 0.25)
    bias = noise(key_of[3], (H,), 0.5, 3.0, (), jnp.float32)
    out_degree = touch_ends(jax.random.randint(key_of[4], (R, NODES), 0, 64), jax.random.fold_in(key_of[4], 1), 0, 63).astype(jnp.int32)
    adjacency = touch_ends((jax.random.randint(key_of[5], (N_DOM, N_FEAT, TILE_DEV, TILE_SIZE, TILE_SIZE), 0, 8) < 1).astype(jnp.int32), jax.random.fold_in(key_of[5], 1), 0, 1)
    tile_index = draw_tile_index(jax.random.fold_in(key_of[8], 71), 0)
    tile_count = draw_tile_count(jax.random.fold_in(key_of[8], 71), 0)
    return dict(node_feats=node_feats, rel_weight=rel_weight, self_weight=self_weight, bias=bias, out_degree=out_degree, adjacency=adjacency, tile_index=tile_index, tile_count=tile_count)


def reference(node_feats, rel_weight, self_weight, bias, out_degree, adjacency, tile_index, tile_count):
    inv_degree = 1.0 / jnp.maximum(out_degree, 1).astype(jnp.float32)

    def transform(relation):
        product = jnp.dot(node_feats, rel_weight[relation], preferred_element_type=jnp.float32)
        return (product * inv_degree[relation][:, None]).astype(jnp.bfloat16)

    messages = lax.map(transform, jnp.arange(R, dtype=jnp.int32))
    flat_tiles = adjacency.reshape(-1, TILE_SIZE, TILE_SIZE)
    flat_index = tile_index.reshape(-1, 3).astype(jnp.int32)
    slot_ids = jnp.arange(TILE_DEV, dtype=jnp.int32)
    live_mask = (slot_ids[None, None, :] < tile_count[:, :, None]).reshape(-1).astype(jnp.float32)
    group_ids = jnp.repeat(jnp.arange(N_DOM, dtype=jnp.int32), N_FEAT * TILE_DEV)

    def accumulate(running, items):
        tile_cells, entry, weight, group = items
        source_row = ((group * BG + entry[2]) * TILE_SIZE).astype(jnp.int32)
        target_row = (entry[1] * TILE_SIZE).astype(jnp.int32)
        source_msg = lax.dynamic_slice(messages, (entry[0].astype(jnp.int32), source_row, jnp.int32(0)), (1, TILE_SIZE, H))[0]
        contribution = jnp.dot(tile_cells.astype(jnp.bfloat16), source_msg, preferred_element_type=jnp.float32) * weight
        current = lax.dynamic_slice_in_dim(running, target_row, TILE_SIZE, 0)
        return lax.dynamic_update_slice_in_dim(running, current + contribution, target_row, 0), None

    start = jnp.zeros((NODES, H), jnp.float32)
    aggregate, unused = lax.scan(accumulate, start, (flat_tiles, flat_index, live_mask, group_ids))
    self_term = jnp.dot(node_feats, self_weight, preferred_element_type=jnp.float32)
    return (aggregate + self_term + bias[None, :]).astype(jnp.bfloat16)
```

```python
import functools

import jax
import jax.numpy as jnp
from jax import lax
from jax.experimental import pallas as pl
from jax.experimental.pallas import tpu as pltpu
from jax.sharding import PartitionSpec as P

MESH = pl.DeviceIdType.MESH
VMEM_LIMIT = 60 * 1024 * 1024


def bit_count(size):
    count = size.bit_length() - 1
    assert 1 << count == size
    return count


def flips(count):
    me = lax.axis_index("feat")
    bits = [(me // (1 << b)) % 2 for b in range(count)]
    return me, bits, [(1 - 2 * bits[b]) * (1 << b) for b in range(count)]


def orders(count, chunks):
    rest = list(range(1, count))
    return [[0] + (rest if c % 2 == 0 else rest[::-1]) for c in range(chunks)]


def greet(feat_partners, dom_partners):
    barrier = pltpu.get_barrier_semaphore()
    dom = lax.axis_index("dom")
    me = lax.axis_index("feat")
    for partner in feat_partners:
        pl.semaphore_signal(barrier, inc=1, device_id=(dom, partner), device_id_type=MESH)
    for partner in dom_partners:
        pl.semaphore_signal(barrier, inc=1, device_id=(partner, me), device_id_type=MESH)
    pl.semaphore_wait(barrier, len(feat_partners) + len(dom_partners))


def message_kernel(
    n, feats_ref, rel_ref, self_ref, bias_ref, degree_ref, msg_ref, own_ref,
    gathered, rel_t, self_t, bias_t, send_sem, recv_sem,
):
    count = bit_count(n)
    relations = rel_ref.shape[0]
    chunks, _, width, tile = gathered.shape
    hidden = n * width
    me, bits, step = flips(count)
    dom = lax.axis_index("dom")
    plan = [order[::-1] for order in orders(count, chunks)]

    for c in range(chunks):
        block = feats_ref[c * tile:(c + 1) * tile, :].astype(jnp.float32)
        gathered[c, me] = block.T.astype(jnp.bfloat16)
    greet([me + step[b] for b in range(count)], [])

    def held(order, stage):
        owners = [me]
        for b in order[:stage]:
            owners = owners + [owner + step[b] for owner in owners]
        return owners

    started = []

    def send(c, stage):
        order = plan[c]
        partner = me + step[order[stage]]
        for i, owner in enumerate(held(order, stage)):
            copy = pltpu.make_async_remote_copy(
                src_ref=gathered.at[c, owner],
                dst_ref=gathered.at[c, owner],
                send_sem=send_sem.at[c, (1 << stage) - 1 + i],
                recv_sem=recv_sem.at[c, (1 << stage) - 1 + i],
                device_id=(dom, partner),
                device_id_type=MESH,
            )
            copy.start()
            started.append(copy)

    def receive(c, stage):
        order = plan[c]
        for i, owner in enumerate(held(order, stage)):
            arrived = owner + step[order[stage]]
            pltpu.make_async_remote_copy(
                src_ref=gathered.at[c, arrived],
                dst_ref=gathered.at[c, arrived],
                send_sem=send_sem.at[c, (1 << stage) - 1 + i],
                recv_sem=recv_sem.at[c, (1 << stage) - 1 + i],
                device_id=(dom, me + step[order[stage]]),
                device_id_type=MESH,
            ).wait_recv()

    for c in range(chunks):
        send(c, 0)
    for r in range(relations):
        rel_t[r] = rel_ref[r].T
    self_t[...] = self_ref[...].T
    bias_t[...] = jnp.broadcast_to(bias_ref[...], (128, hidden)).T
    for stage in range(count):
        for c in range(chunks):
            receive(c, stage)
            if stage + 1 < count:
                send(c, stage + 1)
    self_rows = self_t[pl.ds(pl.multiple_of(me * width, width), width), :]
    bias_column = bias_t[pl.ds(pl.multiple_of(me * width, width), width), :][:, :1]
    for c in range(chunks):
        features = gathered[c].reshape(hidden, tile)
        own_ref[c] = (
            jnp.dot(self_rows, features, preferred_element_type=jnp.float32) + bias_column
        )
        for r in range(relations):
            degree = degree_ref[r:r + 1, c * tile:(c + 1) * tile]
            factor = 1.0 / jnp.maximum(degree, 1).astype(jnp.float32)
            product = jnp.dot(rel_t[r], features, preferred_element_type=jnp.float32)
            msg_ref[r * chunks + c] = (product * factor).astype(jnp.bfloat16)
    for copy in started:
        copy.wait_send()


def tile_kernel(n, chunks, index_ref, count_ref, tiles_ref, msg_ref, out_ref, acc):
    step = pl.program_id(0)
    per_step = tiles_ref.shape[0]
    bits = bit_count(n)
    blocks, hidden, tile = acc.shape
    width = hidden // n

    @pl.when(step == 0)
    def _():
        acc[...] = jnp.zeros_like(acc)

    for i in range(per_step):
        slot = step * per_step + i
        live = (slot < count_ref[0, 0]).astype(jnp.int32)
        message = msg_ref[index_ref[slot, 0] * chunks + index_ref[slot, 2]]
        cells = (tiles_ref[i] * live).astype(jnp.float32).astype(jnp.bfloat16)
        target = index_ref[slot, 1]
        acc[target] += lax.dot_general(
            message, cells, (((1,), (1,)), ((), ())), preferred_element_type=jnp.float32
        )

    @pl.when(step == pl.num_programs(0) - 1)
    def _():
        plan = orders(bits, chunks)

        def write(g, carry):
            for c in range(chunks):
                for f in range(n):
                    place = 0
                    for b in plan[c]:
                        place = place * 2 + (f >> b) % 2
                    part = acc[g * chunks + c, f * width:(f + 1) * width, :]
                    out_ref[c, place, g] = part.astype(jnp.bfloat16)
            return carry

        lax.fori_loop(0, blocks // chunks, write, 0)


def reduce_kernel(n, groups, part_ref, own_ref, out_ref, *scratch):
    count = bit_count(n)
    landed, crossed = scratch[:count], scratch[count]
    send_sem, recv_sem, cross_send, cross_recv = scratch[count + 1:]
    chunks, _, _, width, tile = part_ref.shape
    me, bits, step = flips(count)
    dom = lax.axis_index("dom")
    peers = [lax.rem(dom + k, groups) for k in range(1, groups)]
    plan = orders(count, chunks)
    greet([me + step[b] for b in range(count)], peers)
    started = []

    def source(c, stage):
        return part_ref.at[c] if stage == 0 else landed[stage - 1].at[c]

    def copy_of(c, stage):
        b = plan[c][stage]
        half = n >> (stage + 1)
        return pltpu.make_async_remote_copy(
            src_ref=source(c, stage).at[pl.ds((1 - bits[b]) * half, half)],
            dst_ref=landed[stage].at[c],
            send_sem=send_sem.at[c, stage],
            recv_sem=recv_sem.at[c, stage],
            device_id=(dom, me + step[b]),
            device_id_type=MESH,
        )

    def cross_of(c, k):
        return pltpu.make_async_remote_copy(
            src_ref=landed[count - 1].at[c, 0, peers[k]],
            dst_ref=crossed.at[c, k],
            send_sem=cross_send.at[c, k],
            recv_sem=cross_recv.at[c, k],
            device_id=(peers[k], me),
            device_id_type=MESH,
        )

    def begin(copy):
        copy.start()
        started.append(copy)

    for c in range(chunks):
        begin(copy_of(c, 0))
    for stage in range(count):
        half = n >> (stage + 1)
        for c in range(chunks):
            copy_of(c, stage).wait_recv()
            kept = bits[plan[c][stage]] * half
            for i in range(half):
                def add(g, carry, c=c, i=i, kept=kept, stage=stage):
                    mine = source(c, stage)[kept + i, g].astype(jnp.float32)
                    total = mine + landed[stage][c, i, g].astype(jnp.float32)
                    landed[stage][c, i, g] = total.astype(jnp.bfloat16)
                    return carry

                lax.fori_loop(0, groups, add, 0)
            if stage + 1 < count:
                begin(copy_of(c, stage + 1))
            else:
                for k in range(groups - 1):
                    begin(cross_of(c, k))
    for c in range(chunks):
        total = own_ref[c] + landed[count - 1][c, 0, dom].astype(jnp.float32)
        for k in range(groups - 1):
            cross_of(c, k).wait_recv()
            total = total + crossed[c, k].astype(jnp.float32)
        out_ref[c * tile:(c + 1) * tile, :] = total.T.astype(jnp.bfloat16)
    for copy in started:
        copy.wait_send()


def body(n, groups, node_feats, rel_weight, self_weight, bias, out_degree, adjacency, tile_index, tile_count):
    owned, width = node_feats.shape
    relations, hidden, _ = rel_weight.shape
    slots, tile = adjacency.shape[2], adjacency.shape[-1]
    chunks = owned // tile
    count = bit_count(n)
    whole = pl.BlockSpec(memory_space=pltpu.VMEM)
    messages, own = pl.pallas_call(
        functools.partial(message_kernel, n),
        out_shape=(
            jax.ShapeDtypeStruct((relations * chunks, hidden, tile), jnp.bfloat16),
            jax.ShapeDtypeStruct((chunks, width, tile), jnp.float32),
        ),
        in_specs=[whole] * 5,
        out_specs=(whole, whole),
        scratch_shapes=[
            pltpu.VMEM((chunks, n, width, tile), jnp.bfloat16),
            pltpu.VMEM((relations, hidden, hidden), jnp.bfloat16),
            pltpu.VMEM((hidden, hidden), jnp.bfloat16),
            pltpu.VMEM((hidden, 128), jnp.float32),
            pltpu.SemaphoreType.DMA((chunks, n)),
            pltpu.SemaphoreType.DMA((chunks, n)),
        ],
        compiler_params=pltpu.CompilerParams(
            collective_id=0, has_side_effects=True, vmem_limit_bytes=VMEM_LIMIT
        ),
        name="messages",
    )(node_feats, rel_weight, self_weight, bias[None, :], out_degree)

    per_step = 4 if slots % 4 == 0 else 1
    partial = pl.pallas_call(
        functools.partial(tile_kernel, n, chunks),
        grid=(slots // per_step,),
        out_shape=jax.ShapeDtypeStruct((chunks, n, groups, width, tile), jnp.bfloat16),
        in_specs=[
            pl.BlockSpec(memory_space=pltpu.SMEM),
            pl.BlockSpec(memory_space=pltpu.SMEM),
            pl.BlockSpec((per_step, tile, tile), lambda i: (i, 0, 0)),
            whole,
        ],
        out_specs=whole,
        scratch_shapes=[pltpu.VMEM((groups * chunks, hidden, tile), jnp.float32)],
        compiler_params=pltpu.CompilerParams(vmem_limit_bytes=VMEM_LIMIT),
        name="tiles",
    )(tile_index[0, 0], tile_count, adjacency[0, 0], messages)

    landed = [
        pltpu.VMEM((chunks, n >> (stage + 1), groups, width, tile), jnp.bfloat16)
        for stage in range(count)
    ]
    return pl.pallas_call(
        functools.partial(reduce_kernel, n, groups),
        out_shape=jax.ShapeDtypeStruct((owned, width), jnp.bfloat16),
        in_specs=[whole] * 2,
        out_specs=whole,
        scratch_shapes=landed + [
            pltpu.VMEM((chunks, groups - 1, width, tile), jnp.bfloat16),
            pltpu.SemaphoreType.DMA((chunks, count)),
            pltpu.SemaphoreType.DMA((chunks, count)),
            pltpu.SemaphoreType.DMA((chunks, groups - 1)),
            pltpu.SemaphoreType.DMA((chunks, groups - 1)),
        ],
        compiler_params=pltpu.CompilerParams(
            collective_id=1, has_side_effects=True, vmem_limit_bytes=VMEM_LIMIT
        ),
        name="reduce",
    )(partial, own)


def solution(mesh):
    placed = (
        P("dom", "feat"),
        P(),
        P(),
        P(),
        P(None, "dom"),
        P("dom", "feat", None, None, None),
        P("dom", "feat", None, None),
        P("dom", "feat"),
    )
    return jax.shard_map(
        functools.partial(body, mesh.shape["feat"], mesh.shape["dom"]),
        mesh=mesh, in_specs=placed, out_specs=P("dom", "feat"), check_vma=False,
    )
```

```python
import functools

import jax
import jax.numpy as jnp
from jax import lax
from jax.experimental import pallas as pl
from jax.experimental.pallas import tpu as pltpu
from jax.sharding import PartitionSpec as P

MESH = pl.DeviceIdType.MESH
VMEM_LIMIT = 60 * 1024 * 1024


def bit_count(size):
    count = size.bit_length() - 1
    assert 1 << count == size
    return count


def flips(count):
    me = lax.axis_index("feat")
    bits = [(me // (1 << b)) % 2 for b in range(count)]
    return me, bits, [(1 - 2 * bits[b]) * (1 << b) for b in range(count)]


def orders(count, chunks):
    rest = list(range(1, count))
    return [[0] + (rest if c % 2 == 0 else rest[::-1]) for c in range(chunks)]


def greet(partners):
    barrier = pltpu.get_barrier_semaphore()
    dom = lax.axis_index("dom")
    for partner in partners:
        pl.semaphore_signal(barrier, inc=1, device_id=(dom, partner), device_id_type=MESH)
    pl.semaphore_wait(barrier, len(partners))


def message_kernel(
    n, feats_ref, rel_ref, self_ref, bias_ref, degree_ref, msg_ref, own_ref,
    gathered, rel_t, self_t, bias_t, send_sem, recv_sem,
):
    count = bit_count(n)
    relations = rel_ref.shape[0]
    chunks, _, width, tile = gathered.shape
    hidden = n * width
    me, bits, step = flips(count)
    dom = lax.axis_index("dom")
    plan = [order[::-1] for order in orders(count, chunks)]

    for c in range(chunks):
        gathered[c, me] = feats_ref[:, c * tile:(c + 1) * tile]
    greet([me + step[b] for b in range(count)])

    def held(order, stage):
        owners = [me]
        for b in order[:stage]:
            owners = owners + [owner + step[b] for owner in owners]
        return owners

    started = []

    def send(c, stage):
        order = plan[c]
        partner = me + step[order[stage]]
        for i, owner in enumerate(held(order, stage)):
            copy = pltpu.make_async_remote_copy(
                src_ref=gathered.at[c, owner],
                dst_ref=gathered.at[c, owner],
                send_sem=send_sem.at[c, (1 << stage) - 1 + i],
                recv_sem=recv_sem.at[c, (1 << stage) - 1 + i],
                device_id=(dom, partner),
                device_id_type=MESH,
            )
            copy.start()
            started.append(copy)

    def receive(c, stage):
        order = plan[c]
        for i, owner in enumerate(held(order, stage)):
            arrived = owner + step[order[stage]]
            pltpu.make_async_remote_copy(
                src_ref=gathered.at[c, arrived],
                dst_ref=gathered.at[c, arrived],
                send_sem=send_sem.at[c, (1 << stage) - 1 + i],
                recv_sem=recv_sem.at[c, (1 << stage) - 1 + i],
                device_id=(dom, me + step[order[stage]]),
                device_id_type=MESH,
            ).wait_recv()

    for c in range(chunks):
        send(c, 0)
    for r in range(relations):
        rel_t[r] = rel_ref[r].T
    self_t[...] = self_ref[...].T
    bias_t[...] = jnp.broadcast_to(bias_ref[...], (128, hidden)).T
    self_rows = self_t[pl.ds(pl.multiple_of(me * width, width), width), :]
    bias_column = bias_t[pl.ds(pl.multiple_of(me * width, width), width), :][:, :1]
    for stage in range(count):
        for c in range(chunks):
            receive(c, stage)
            if stage + 1 < count:
                send(c, stage + 1)
                continue
            features = gathered[c].reshape(hidden, tile)
            own_ref[c] = (
                jnp.dot(self_rows, features, preferred_element_type=jnp.float32) + bias_column
            )
            for r in range(relations):
                degree = degree_ref[r:r + 1, c * tile:(c + 1) * tile]
                factor = 1.0 / jnp.maximum(degree, 1).astype(jnp.float32)
                product = jnp.dot(rel_t[r], features, preferred_element_type=jnp.float32)
                msg_ref[r * chunks + c] = (product * factor).astype(jnp.bfloat16)
    for copy in started:
        copy.wait_send()


def reduce_orders(n, groups, chunks):
    rest = [("feat", b) for b in range(1, bit_count(n))]
    last = [("dom", b) for b in range(bit_count(groups))]
    rest, last = rest + last[:1], last[1:]
    plans = []
    for c in range(chunks):
        k = c % max(len(rest), 1)
        plans.append([("feat", 0)] + rest[k:] + rest[:k] + last)
    return plans


def tile_kernel(n, groups, chunks, index_ref, count_ref, tiles_ref, msg_ref, sent_ref, kept_ref, acc):
    step = pl.program_id(0)
    per_step = tiles_ref.shape[0]
    blocks, hidden, tile = acc.shape
    sources = blocks // groups
    width = hidden // n
    lanes = sent_ref.shape[-1]
    pieces = tile // lanes
    parity = lax.rem(lax.axis_index("feat"), 2)

    @pl.when(step == 0)
    def _():
        acc[...] = jnp.zeros_like(acc)

    for i in range(per_step):
        slot = step * per_step + i
        live = (slot < count_ref[0, 0]).astype(jnp.int32)
        message = msg_ref[index_ref[0, 0, slot] * sources + index_ref[2, 0, slot]]
        cells = (tiles_ref[i] * live).astype(jnp.float32).astype(jnp.bfloat16)
        target = index_ref[1, 0, slot]
        acc[target] += lax.dot_general(
            message, cells, (((1,), (1,)), ((), ())), preferred_element_type=jnp.float32
        )

    @pl.when(step == pl.num_programs(0) - 1)
    def _():
        plans = reduce_orders(n, groups, chunks)
        for c in range(chunks):
            s, piece = c // pieces, c % pieces
            for g in range(groups):
                for f in range(0, n, 2):
                    place = 0
                    for axis, b in plans[c][1:]:
                        place = place * 2 + ((f if axis == "feat" else g) >> b) % 2
                    for ref, core in ((sent_ref, 1 - parity), (kept_ref, parity)):
                        start = pl.multiple_of((f + core) * width, width)
                        part = acc[
                            g * sources + s, pl.ds(start, width),
                            piece * lanes:(piece + 1) * lanes,
                        ]
                        ref[c, place] = part.astype(ref.dtype)


def reduce_kernel(n, groups, first_ref, kept_ref, own_ref, out_ref, total, *scratch):
    plans = reduce_orders(n, groups, first_ref.shape[0])
    stages = len(plans[0])
    landed, sent = scratch[:stages], (first_ref,) + scratch[stages:2 * stages - 1]
    send_sem, recv_sem = scratch[2 * stages - 1:]
    chunks, half_all, width, lanes = first_ref.shape
    tile = own_ref.shape[-1]
    pieces = tile // lanes
    me, dom = lax.axis_index("feat"), lax.axis_index("dom")

    def bit(axis, b):
        return ((me if axis == "feat" else dom) // (1 << b)) % 2

    def partner(axis, b):
        move = (1 - 2 * bit(axis, b)) * (1 << b)
        return (dom, me + move) if axis == "feat" else (dom + move, me)

    barrier = pltpu.get_barrier_semaphore()
    for axis, b in plans[0]:
        pl.semaphore_signal(barrier, inc=1, device_id=partner(axis, b), device_id_type=MESH)
    pl.semaphore_wait(barrier, stages)

    def copy_of(c, stage):
        return pltpu.make_async_remote_copy(
            src_ref=sent[stage].at[c],
            dst_ref=landed[stage].at[c],
            send_sem=send_sem.at[c, stage],
            recv_sem=recv_sem.at[c, stage],
            device_id=partner(*plans[c][stage]),
            device_id_type=MESH,
        )

    def arrived(stage, c, i):
        return landed[stage][c, i].astype(jnp.float32)

    for c in range(chunks):
        copy_of(c, 0).start()
    base = [0] * chunks
    for stage in range(stages):
        source = kept_ref if stage == 0 else total
        half = half_all >> (stage + 1)
        for c in range(chunks):
            copy_of(c, stage).wait_recv()
            if stage + 1 < stages:
                mine = bit(*plans[c][stage + 1])
                away = (1 - mine) * half
                stay = mine * half

                def give(i, carry, c=c, stage=stage, away=away, source=source):
                    value = source[c, base[c] + away + i] + arrived(stage, c, away + i)
                    sent[stage + 1][c, i] = value.astype(jnp.bfloat16)
                    return carry

                def keep(i, carry, c=c, stage=stage, stay=stay, source=source):
                    place = base[c] + stay + i
                    total[c, place] = source[c, place] + arrived(stage, c, stay + i)
                    return carry

                lax.fori_loop(0, half, give, 0, unroll=min(half, 4))
                copy_of(c, stage + 1).start()
                lax.fori_loop(0, half, keep, 0, unroll=min(half, 4))
                base[c] = base[c] + stay
            else:
                s, piece = c // pieces, c % pieces
                value = source[c, base[c]] + arrived(stage, c, 0)
                value = value + own_ref[s, :, piece * lanes:(piece + 1) * lanes]
                out_ref[:, c * lanes:(c + 1) * lanes] = value.astype(jnp.bfloat16)
    for stage in range(stages):
        for c in range(chunks):
            copy_of(c, stage).wait_send()


def body(n, groups, node_feats, rel_weight, self_weight, bias, out_degree, adjacency, tile_index, tile_count):
    owned, width = node_feats.shape
    relations, hidden, _ = rel_weight.shape
    slots, tile = adjacency.shape[2], adjacency.shape[-1]
    chunks = owned // tile
    count = bit_count(n)
    whole = pl.BlockSpec(memory_space=pltpu.VMEM)
    messages, own = pl.pallas_call(
        functools.partial(message_kernel, n),
        out_shape=(
            jax.ShapeDtypeStruct((relations * chunks, hidden, tile), jnp.bfloat16),
            jax.ShapeDtypeStruct((chunks, width, tile), jnp.float32),
        ),
        in_specs=[whole] * 5,
        out_specs=(whole, whole),
        scratch_shapes=[
            pltpu.VMEM((chunks, n, width, tile), jnp.bfloat16),
            pltpu.VMEM((relations, hidden, hidden), jnp.bfloat16),
            pltpu.VMEM((hidden, hidden), jnp.bfloat16),
            pltpu.VMEM((hidden, 128), jnp.float32),
            pltpu.SemaphoreType.DMA((chunks, n)),
            pltpu.SemaphoreType.DMA((chunks, n)),
        ],
        compiler_params=pltpu.CompilerParams(
            collective_id=0, has_side_effects=True, vmem_limit_bytes=VMEM_LIMIT
        ),
        name="messages",
    )(node_feats.T, rel_weight, self_weight, bias[None, :], out_degree)

    per_step = 4 if slots % 4 == 0 else 1
    lanes = tile // 2
    pieces = chunks * (tile // lanes)
    half = n * groups // 2
    sent, kept = pl.pallas_call(
        functools.partial(tile_kernel, n, groups, pieces),
        grid=(slots // per_step,),
        out_shape=(
            jax.ShapeDtypeStruct((pieces, half, width, lanes), jnp.bfloat16),
            jax.ShapeDtypeStruct((pieces, half, width, lanes), jnp.float32),
        ),
        in_specs=[
            pl.BlockSpec(memory_space=pltpu.SMEM),
            pl.BlockSpec(memory_space=pltpu.SMEM),
            pl.BlockSpec((per_step, tile, tile), lambda i: (i, 0, 0)),
            whole,
        ],
        out_specs=(whole, whole),
        scratch_shapes=[pltpu.VMEM((groups * chunks, hidden, tile), jnp.float32)],
        compiler_params=pltpu.CompilerParams(vmem_limit_bytes=VMEM_LIMIT),
        name="tiles",
    )(jnp.transpose(tile_index[0], (2, 0, 1)), tile_count, adjacency[0, 0], messages)

    stages = bit_count(n * groups)
    halves = [
        pltpu.VMEM((pieces, half >> stage, width, lanes), jnp.bfloat16)
        for stage in range(stages)
    ]
    result = pl.pallas_call(
        functools.partial(reduce_kernel, n, groups),
        out_shape=jax.ShapeDtypeStruct((width, owned), jnp.bfloat16),
        in_specs=[whole] * 3,
        out_specs=whole,
        scratch_shapes=[pltpu.VMEM((pieces, half, width, lanes), jnp.float32)]
        + halves + halves[1:] + [
            pltpu.SemaphoreType.DMA((pieces, stages)),
            pltpu.SemaphoreType.DMA((pieces, stages)),
        ],
        compiler_params=pltpu.CompilerParams(
            collective_id=1, has_side_effects=True, vmem_limit_bytes=VMEM_LIMIT
        ),
        name="reduce",
    )(sent, kept, own)
    return result.T


def solution(mesh):
    placed = (
        P("dom", "feat"),
        P(),
        P(),
        P(),
        P(None, "dom"),
        P("dom", "feat", None, None, None),
        P("dom", "feat", None, None),
        P("dom", "feat"),
    )
    return jax.shard_map(
        functools.partial(body, mesh.shape["feat"], mesh.shape["dom"]),
        mesh=mesh, in_specs=placed, out_specs=P("dom", "feat"), check_vma=False,
    )
```

```python
import functools

import jax
import jax.numpy as jnp
from jax import lax
from jax.experimental import pallas as pl
from jax.experimental.pallas import tpu as pltpu
from jax.sharding import PartitionSpec as P

MESH = pl.DeviceIdType.MESH
VMEM_LIMIT = 28 * 1024 * 1024


def bit_count(size):
    count = size.bit_length() - 1
    assert 1 << count == size
    return count


def flips(count):
    me = lax.axis_index("feat")
    bits = [(me // (1 << b)) % 2 for b in range(count)]
    return me, bits, [(1 - 2 * bits[b]) * (1 << b) for b in range(count)]


def orders(count, chunks):
    rest = list(range(1, count))
    return [[0] + (rest if c % 2 == 0 else rest[::-1]) for c in range(chunks)]


def greet(partners):
    barrier = pltpu.get_barrier_semaphore()
    dom = lax.axis_index("dom")
    for partner in partners:
        pl.semaphore_signal(barrier, inc=1, device_id=(dom, partner), device_id_type=MESH)
    pl.semaphore_wait(barrier, len(partners))


def message_kernel(
    n, feats_ref, rel_ref, self_ref, bias_ref, degree_ref, msg_ref, own_ref,
    gathered, rel_t, self_t, bias_t, send_sem, recv_sem,
):
    count = bit_count(n)
    relations = rel_ref.shape[0]
    chunks, _, width, tile = gathered.shape
    hidden = n * width
    me, bits, step = flips(count)
    dom = lax.axis_index("dom")
    plan = [order[::-1] for order in orders(count, chunks)]

    for c in range(chunks):
        gathered[c, me] = feats_ref[:, c * tile:(c + 1) * tile]
    greet([me + step[b] for b in range(count)])

    def held(order, stage):
        owners = [me]
        for b in order[:stage]:
            owners = owners + [owner + step[b] for owner in owners]
        return owners

    started = []

    def send(c, stage):
        order = plan[c]
        partner = me + step[order[stage]]
        for i, owner in enumerate(held(order, stage)):
            copy = pltpu.make_async_remote_copy(
                src_ref=gathered.at[c, owner],
                dst_ref=gathered.at[c, owner],
                send_sem=send_sem.at[c, (1 << stage) - 1 + i],
                recv_sem=recv_sem.at[c, (1 << stage) - 1 + i],
                device_id=(dom, partner),
                device_id_type=MESH,
            )
            copy.start()
            started.append(copy)

    def receive(c, stage):
        order = plan[c]
        for i, owner in enumerate(held(order, stage)):
            arrived = owner + step[order[stage]]
            pltpu.make_async_remote_copy(
                src_ref=gathered.at[c, arrived],
                dst_ref=gathered.at[c, arrived],
                send_sem=send_sem.at[c, (1 << stage) - 1 + i],
                recv_sem=recv_sem.at[c, (1 << stage) - 1 + i],
                device_id=(dom, me + step[order[stage]]),
                device_id_type=MESH,
            ).wait_recv()

    for c in range(chunks):
        send(c, 0)
    for r in range(relations):
        rel_t[r] = rel_ref[r].T
    self_t[...] = self_ref[...].T
    bias_t[...] = jnp.broadcast_to(bias_ref[...], (128, hidden)).T
    self_rows = self_t[pl.ds(pl.multiple_of(me * width, width), width), :]
    bias_column = bias_t[pl.ds(pl.multiple_of(me * width, width), width), :][:, :1]
    for stage in range(count):
        for c in range(chunks):
            receive(c, stage)
            if stage + 1 < count:
                send(c, stage + 1)
                continue
            features = gathered[c].reshape(hidden, tile)
            own_ref[c] = (
                jnp.dot(self_rows, features, preferred_element_type=jnp.float32) + bias_column
            )
            for r in range(relations):
                degree = degree_ref[r:r + 1, c * tile:(c + 1) * tile]
                factor = 1.0 / jnp.maximum(degree, 1).astype(jnp.float32)
                product = jnp.dot(rel_t[r], features, preferred_element_type=jnp.float32)
                msg_ref[r * chunks + c] = (product * factor).astype(jnp.bfloat16)
    for copy in started:
        copy.wait_send()


def reduce_orders(n, groups, chunks):
    rest = [("feat", b) for b in range(1, bit_count(n))]
    last = [("dom", b) for b in range(bit_count(groups))]
    rest, last = rest + last[:1], last[1:]
    plans = []
    for c in range(chunks):
        k = c % max(len(rest), 1)
        plans.append([("feat", 0)] + rest[k:] + rest[:k] + last)
    return plans


def tile_kernel(n, groups, chunks, index_ref, count_ref, tiles_ref, msg_ref, sent_ref, kept_ref, acc):
    step = pl.program_id(0)
    per_step = tiles_ref.shape[0]
    blocks, hidden, tile = acc.shape
    sources = blocks // groups
    width = hidden // n
    lanes = sent_ref.shape[-1]
    pieces = tile // lanes
    parity = lax.rem(lax.axis_index("feat"), 2)

    @pl.when(step == 0)
    def _():
        acc[...] = jnp.zeros_like(acc)

    for i in range(per_step):
        slot = step * per_step + i
        live = (slot < count_ref[0, 0]).astype(jnp.int32)
        message = msg_ref[index_ref[0, 0, slot] * sources + index_ref[2, 0, slot]]
        cells = (tiles_ref[i] * live).astype(jnp.float32).astype(jnp.bfloat16)
        target = index_ref[1, 0, slot]
        acc[target] += lax.dot_general(
            message, cells, (((1,), (1,)), ((), ())), preferred_element_type=jnp.float32
        )

    @pl.when(step == pl.num_programs(0) - 1)
    def _():
        plans = reduce_orders(n, groups, chunks)
        for c in range(chunks):
            s, piece = c // pieces, c % pieces
            for g in range(groups):
                for f in range(0, n, 2):
                    place = 0
                    for axis, b in plans[c][1:]:
                        place = place * 2 + ((f if axis == "feat" else g) >> b) % 2
                    for ref, core in ((sent_ref, 1 - parity), (kept_ref, parity)):
                        start = pl.multiple_of((f + core) * width, width)
                        part = acc[
                            g * sources + s, pl.ds(start, width),
                            piece * lanes:(piece + 1) * lanes,
                        ]
                        ref[c, place] = part.astype(ref.dtype)


def reduce_kernel(n, groups, first_ref, kept_ref, own_ref, out_ref, total, *scratch):
    plans = reduce_orders(n, groups, first_ref.shape[0])
    stages = len(plans[0])
    landed, sent = scratch[:stages], (first_ref,) + scratch[stages:2 * stages - 1]
    send_sem, recv_sem = scratch[2 * stages - 1:]
    chunks, half_all, width, lanes = first_ref.shape
    tile = own_ref.shape[-1]
    pieces = tile // lanes
    me, dom = lax.axis_index("feat"), lax.axis_index("dom")

    def bit(axis, b):
        return ((me if axis == "feat" else dom) // (1 << b)) % 2

    def partner(axis, b):
        move = (1 - 2 * bit(axis, b)) * (1 << b)
        return (dom, me + move) if axis == "feat" else (dom + move, me)

    barrier = pltpu.get_barrier_semaphore()
    for axis, b in plans[0]:
        pl.semaphore_signal(barrier, inc=1, device_id=partner(axis, b), device_id_type=MESH)
    pl.semaphore_wait(barrier, stages)

    def copy_of(c, stage):
        return pltpu.make_async_remote_copy(
            src_ref=sent[stage].at[c],
            dst_ref=landed[stage].at[c],
            send_sem=send_sem.at[c, stage],
            recv_sem=recv_sem.at[c, stage],
            device_id=partner(*plans[c][stage]),
            device_id_type=MESH,
        )

    def arrived(stage, c, i):
        return landed[stage][c, i].astype(jnp.float32)

    for c in range(chunks):
        copy_of(c, 0).start()
    base = [0] * chunks
    for stage in range(stages):
        source = kept_ref if stage == 0 else total
        half = half_all >> (stage + 1)
        for c in range(chunks):
            copy_of(c, stage).wait_recv()
            if stage + 1 < stages:
                mine = bit(*plans[c][stage + 1])
                away = (1 - mine) * half
                stay = mine * half

                def give(i, carry, c=c, stage=stage, away=away, source=source):
                    value = source[c, base[c] + away + i] + arrived(stage, c, away + i)
                    sent[stage + 1][c, i] = value.astype(jnp.bfloat16)
                    return carry

                def keep(i, carry, c=c, stage=stage, stay=stay, source=source):
                    place = base[c] + stay + i
                    total[c, place] = source[c, place] + arrived(stage, c, stay + i)
                    return carry

                lax.fori_loop(0, half, give, 0, unroll=min(half, 4))
                copy_of(c, stage + 1).start()
                lax.fori_loop(0, half, keep, 0, unroll=min(half, 4))
                base[c] = base[c] + stay
            else:
                s, piece = c // pieces, c % pieces
                value = source[c, base[c]] + arrived(stage, c, 0)
                value = value + own_ref[s, :, piece * lanes:(piece + 1) * lanes]
                out_ref[:, c * lanes:(c + 1) * lanes] = value.astype(jnp.bfloat16)
    for stage in range(stages):
        for c in range(chunks):
            copy_of(c, stage).wait_send()


def body(n, groups, node_feats, rel_weight, self_weight, bias, out_degree, adjacency, tile_index, tile_count):
    owned, width = node_feats.shape
    relations, hidden, _ = rel_weight.shape
    slots, tile = adjacency.shape[2], adjacency.shape[-1]
    chunks = owned // tile
    count = bit_count(n)
    whole = pl.BlockSpec(memory_space=pltpu.VMEM)
    messages, own = pl.pallas_call(
        functools.partial(message_kernel, n),
        out_shape=(
            pltpu.VMEM((relations * chunks, hidden, tile), jnp.bfloat16),
            pltpu.VMEM((chunks, width, tile), jnp.float32),
        ),
        in_specs=[whole] * 5,
        out_specs=(whole, whole),
        scratch_shapes=[
            pltpu.VMEM((chunks, n, width, tile), jnp.bfloat16),
            pltpu.VMEM((relations, hidden, hidden), jnp.bfloat16),
            pltpu.VMEM((hidden, hidden), jnp.bfloat16),
            pltpu.VMEM((hidden, 128), jnp.float32),
            pltpu.SemaphoreType.DMA((chunks, n)),
            pltpu.SemaphoreType.DMA((chunks, n)),
        ],
        compiler_params=pltpu.CompilerParams(
            collective_id=0, has_side_effects=True, vmem_limit_bytes=VMEM_LIMIT
        ),
        name="messages",
    )(node_feats.T, rel_weight, self_weight, bias[None, :], out_degree)

    per_step = next(p for p in (8, 4, 2, 1) if slots % p == 0)
    lanes = tile // 2
    pieces = chunks * (tile // lanes)
    half = n * groups // 2
    sent, kept = pl.pallas_call(
        functools.partial(tile_kernel, n, groups, pieces),
        grid=(slots // per_step,),
        out_shape=(
            pltpu.VMEM((pieces, half, width, lanes), jnp.bfloat16),
            pltpu.VMEM((pieces, half, width, lanes), jnp.float32),
        ),
        in_specs=[
            pl.BlockSpec(memory_space=pltpu.SMEM),
            pl.BlockSpec(memory_space=pltpu.SMEM),
            pl.BlockSpec((per_step, tile, tile), lambda i: (i, 0, 0)),
            whole,
        ],
        out_specs=(whole, whole),
        scratch_shapes=[pltpu.VMEM((groups * chunks, hidden, tile), jnp.float32)],
        compiler_params=pltpu.CompilerParams(vmem_limit_bytes=VMEM_LIMIT),
        name="tiles",
    )(jnp.transpose(tile_index[0], (2, 0, 1)), tile_count, adjacency[0, 0], messages)

    stages = bit_count(n * groups)
    halves = [
        pltpu.VMEM((pieces, half >> stage, width, lanes), jnp.bfloat16)
        for stage in range(stages)
    ]
    result = pl.pallas_call(
        functools.partial(reduce_kernel, n, groups),
        out_shape=jax.ShapeDtypeStruct((width, owned), jnp.bfloat16),
        in_specs=[whole] * 3,
        out_specs=whole,
        scratch_shapes=[pltpu.VMEM((pieces, half, width, lanes), jnp.float32)]
        + halves + halves[1:] + [
            pltpu.SemaphoreType.DMA((pieces, stages)),
            pltpu.SemaphoreType.DMA((pieces, stages)),
        ],
        compiler_params=pltpu.CompilerParams(
            collective_id=1, has_side_effects=True, vmem_limit_bytes=VMEM_LIMIT
        ),
        name="reduce",
    )(sent, kept, own)
    return result.T


def solution(mesh):
    placed = (
        P("dom", "feat"),
        P(),
        P(),
        P(),
        P(None, "dom"),
        P("dom", "feat", None, None, None),
        P("dom", "feat", None, None),
        P("dom", "feat"),
    )
    return jax.shard_map(
        functools.partial(body, mesh.shape["feat"], mesh.shape["dom"]),
        mesh=mesh, in_specs=placed, out_specs=P("dom", "feat"), check_vma=False,
    )
```

```python
import functools

import jax
import jax.numpy as jnp
from jax import lax
from jax.experimental import pallas as pl
from jax.experimental.pallas import tpu as pltpu
from jax.sharding import PartitionSpec as P

MESH = pl.DeviceIdType.MESH
VMEM_LIMIT = 28 * 1024 * 1024


def bit_count(size):
    count = size.bit_length() - 1
    assert 1 << count == size
    return count


def flips(count):
    me = lax.axis_index("feat")
    bits = [(me // (1 << b)) % 2 for b in range(count)]
    return me, bits, [(1 - 2 * bits[b]) * (1 << b) for b in range(count)]


def orders(count, chunks):
    rest = list(range(1, count))
    return [[0] + (rest if c % 2 == 0 else rest[::-1]) for c in range(chunks)]


def greet(partners):
    barrier = pltpu.get_barrier_semaphore()
    dom = lax.axis_index("dom")
    for partner in partners:
        pl.semaphore_signal(barrier, inc=1, device_id=(dom, partner), device_id_type=MESH)
    pl.semaphore_wait(barrier, len(partners))


def message_kernel(
    n, feats_ref, rel_ref, self_ref, bias_ref, degree_ref, msg_ref, own_ref,
    gathered, rel_t, self_t, bias_t, send_sem, recv_sem,
):
    count = bit_count(n)
    relations = rel_ref.shape[0]
    chunks, _, width, tile = gathered.shape
    hidden = n * width
    me, bits, step = flips(count)
    dom = lax.axis_index("dom")
    plan = [order[::-1] for order in orders(count, chunks)]

    for c in range(chunks):
        gathered[c, me] = feats_ref[:, c * tile:(c + 1) * tile]
    greet([me + step[b] for b in range(count)])

    def held(order, stage):
        owners = [me]
        for b in order[:stage]:
            owners = owners + [owner + step[b] for owner in owners]
        return owners

    started = []

    def send(c, stage):
        order = plan[c]
        partner = me + step[order[stage]]
        for i, owner in enumerate(held(order, stage)):
            copy = pltpu.make_async_remote_copy(
                src_ref=gathered.at[c, owner],
                dst_ref=gathered.at[c, owner],
                send_sem=send_sem.at[c, (1 << stage) - 1 + i],
                recv_sem=recv_sem.at[c, (1 << stage) - 1 + i],
                device_id=(dom, partner),
                device_id_type=MESH,
            )
            copy.start()
            started.append(copy)

    def receive(c, stage):
        order = plan[c]
        for i, owner in enumerate(held(order, stage)):
            arrived = owner + step[order[stage]]
            pltpu.make_async_remote_copy(
                src_ref=gathered.at[c, arrived],
                dst_ref=gathered.at[c, arrived],
                send_sem=send_sem.at[c, (1 << stage) - 1 + i],
                recv_sem=recv_sem.at[c, (1 << stage) - 1 + i],
                device_id=(dom, me + step[order[stage]]),
                device_id_type=MESH,
            ).wait_recv()

    for c in range(chunks):
        send(c, 0)
    for r in range(relations):
        rel_t[r] = rel_ref[r].T
    self_t[...] = self_ref[...].T
    bias_t[...] = jnp.broadcast_to(bias_ref[...], (128, hidden)).T
    self_rows = self_t[pl.ds(pl.multiple_of(me * width, width), width), :]
    bias_column = bias_t[pl.ds(pl.multiple_of(me * width, width), width), :][:, :1]
    for stage in range(count):
        for c in range(chunks):
            receive(c, stage)
            if stage + 1 < count:
                send(c, stage + 1)
                continue
            features = gathered[c].reshape(hidden, tile)
            own_ref[c] = (
                jnp.dot(self_rows, features, preferred_element_type=jnp.float32) + bias_column
            )
            for r in range(relations):
                degree = degree_ref[r:r + 1, c * tile:(c + 1) * tile]
                factor = 1.0 / jnp.maximum(degree, 1).astype(jnp.float32)
                product = jnp.dot(rel_t[r], features, preferred_element_type=jnp.float32)
                msg_ref[r * chunks + c] = (product * factor).astype(jnp.bfloat16)
    for copy in started:
        copy.wait_send()


def reduce_orders(n, groups, chunks):
    rest = [("feat", b) for b in range(1, bit_count(n))]
    last = [("dom", b) for b in range(bit_count(groups))]
    rest, last = rest + last[:1], last[1:]
    plans = []
    for c in range(chunks):
        k = c % max(len(rest), 1)
        plans.append([("feat", 0)] + rest[k:] + rest[:k] + last)
    return plans


def tile_kernel(n, groups, chunks, index_ref, count_ref, tiles_ref, msg_ref, sent_ref, kept_ref, acc):
    step = pl.program_id(0)
    per_step = tiles_ref.shape[0]
    blocks, hidden, tile = acc.shape
    sources = blocks // groups
    width = hidden // n
    lanes = sent_ref.shape[-1]
    pieces = tile // lanes
    parity = lax.rem(lax.axis_index("feat"), 2)

    @pl.when(step == 0)
    def _():
        acc[...] = jnp.zeros_like(acc)

    for i in range(per_step):
        slot = step * per_step + i
        live = (slot < count_ref[0, 0]).astype(jnp.int32)
        message = msg_ref[index_ref[0, 0, slot] * sources + index_ref[2, 0, slot]]
        cells = (tiles_ref[i] * live).astype(jnp.float32).astype(jnp.bfloat16)
        target = index_ref[1, 0, slot]
        acc[target] += lax.dot_general(
            message, cells, (((1,), (1,)), ((), ())), preferred_element_type=jnp.float32
        )

    @pl.when(step == pl.num_programs(0) - 1)
    def _():
        plans = reduce_orders(n, groups, chunks)
        for c in range(chunks):
            s, piece = c // pieces, c % pieces
            for g in range(groups):
                for f in range(0, n, 2):
                    place = 0
                    for axis, b in plans[c][1:]:
                        place = place * 2 + ((f if axis == "feat" else g) >> b) % 2
                    for ref, core in ((sent_ref, 1 - parity), (kept_ref, parity)):
                        start = pl.multiple_of((f + core) * width, width)
                        part = acc[
                            g * sources + s, pl.ds(start, width),
                            piece * lanes:(piece + 1) * lanes,
                        ]
                        ref[c, place] = part.astype(ref.dtype)


def reduce_kernel(n, groups, first_ref, kept_ref, own_ref, out_ref, total, *scratch):
    plans = reduce_orders(n, groups, first_ref.shape[0])
    stages = len(plans[0])
    landed, sent = scratch[:stages], (first_ref,) + scratch[stages:2 * stages - 1]
    send_sem, recv_sem = scratch[2 * stages - 1:]
    chunks, half_all, width, lanes = first_ref.shape
    tile = own_ref.shape[-1]
    pieces = tile // lanes
    me, dom = lax.axis_index("feat"), lax.axis_index("dom")

    def bit(axis, b):
        return ((me if axis == "feat" else dom) // (1 << b)) % 2

    def partner(axis, b):
        move = (1 - 2 * bit(axis, b)) * (1 << b)
        return (dom, me + move) if axis == "feat" else (dom + move, me)

    barrier = pltpu.get_barrier_semaphore()
    for axis, b in plans[0]:
        pl.semaphore_signal(barrier, inc=1, device_id=partner(axis, b), device_id_type=MESH)
    pl.semaphore_wait(barrier, stages)

    def copy_of(c, stage):
        return pltpu.make_async_remote_copy(
            src_ref=sent[stage].at[c],
            dst_ref=landed[stage].at[c],
            send_sem=send_sem.at[c, stage],
            recv_sem=recv_sem.at[c, stage],
            device_id=partner(*plans[c][stage]),
            device_id_type=MESH,
        )

    def arrived(stage, c, i):
        return landed[stage][c, i].astype(jnp.float32)

    for c in range(chunks):
        copy_of(c, 0).start()
    base = [0] * chunks
    for stage in range(stages):
        source = kept_ref if stage == 0 else total
        half = half_all >> (stage + 1)
        for c in range(chunks):
            copy_of(c, stage).wait_recv()
            if stage + 1 < stages:
                mine = bit(*plans[c][stage + 1])
                away = (1 - mine) * half
                stay = mine * half

                def give(i, carry, c=c, stage=stage, away=away, source=source):
                    value = source[c, base[c] + away + i] + arrived(stage, c, away + i)
                    sent[stage + 1][c, i] = value.astype(jnp.bfloat16)
                    return carry

                def keep(i, carry, c=c, stage=stage, stay=stay, source=source):
                    place = base[c] + stay + i
                    total[c, place] = source[c, place] + arrived(stage, c, stay + i)
                    return carry

                lax.fori_loop(0, half, give, 0, unroll=min(half, 4))
                copy_of(c, stage + 1).start()
                lax.fori_loop(0, half, keep, 0, unroll=min(half, 4))
                base[c] = base[c] + stay
            else:
                s, piece = c // pieces, c % pieces
                value = source[c, base[c]] + arrived(stage, c, 0)
                value = value + own_ref[s, :, piece * lanes:(piece + 1) * lanes]
                out_ref[:, c * lanes:(c + 1) * lanes] = value.astype(jnp.bfloat16)
    for stage in range(stages):
        for c in range(chunks):
            copy_of(c, stage).wait_send()


def body(n, groups, node_feats, rel_weight, self_weight, bias, out_degree, adjacency, tile_index, tile_count):
    owned, width = node_feats.shape
    relations, hidden, _ = rel_weight.shape
    slots, tile = adjacency.shape[2], adjacency.shape[-1]
    chunks = owned // tile
    count = bit_count(n)
    whole = pl.BlockSpec(memory_space=pltpu.VMEM)
    messages, own = pl.pallas_call(
        functools.partial(message_kernel, n),
        out_shape=(
            pltpu.VMEM((relations * chunks, hidden, tile), jnp.bfloat16),
            pltpu.VMEM((chunks, width, tile), jnp.float32),
        ),
        in_specs=[whole] * 5,
        out_specs=(whole, whole),
        scratch_shapes=[
            pltpu.VMEM((chunks, n, width, tile), jnp.bfloat16),
            pltpu.VMEM((relations, hidden, hidden), jnp.bfloat16),
            pltpu.VMEM((hidden, hidden), jnp.bfloat16),
            pltpu.VMEM((hidden, 128), jnp.float32),
            pltpu.SemaphoreType.DMA((chunks, n)),
            pltpu.SemaphoreType.DMA((chunks, n)),
        ],
        compiler_params=pltpu.CompilerParams(
            collective_id=0, has_side_effects=True, vmem_limit_bytes=VMEM_LIMIT
        ),
        name="messages",
    )(*[
        pltpu.with_memory_space_constraint(x, pltpu.HBM)
        for x in (node_feats.T, rel_weight, self_weight, bias[None, :], out_degree)
    ])

    per_step = next(p for p in (8, 4, 2, 1) if slots % p == 0)
    lanes = tile // 2
    pieces = chunks * (tile // lanes)
    half = n * groups // 2
    sent, kept = pl.pallas_call(
        functools.partial(tile_kernel, n, groups, pieces),
        grid=(slots // per_step,),
        out_shape=(
            pltpu.VMEM((pieces, half, width, lanes), jnp.bfloat16),
            pltpu.VMEM((pieces, half, width, lanes), jnp.float32),
        ),
        in_specs=[
            pl.BlockSpec(memory_space=pltpu.SMEM),
            pl.BlockSpec(memory_space=pltpu.SMEM),
            pl.BlockSpec((per_step, tile, tile), lambda i: (i, 0, 0)),
            whole,
        ],
        out_specs=(whole, whole),
        scratch_shapes=[pltpu.VMEM((groups * chunks, hidden, tile), jnp.float32)],
        compiler_params=pltpu.CompilerParams(vmem_limit_bytes=VMEM_LIMIT),
        name="tiles",
    )(jnp.transpose(tile_index[0], (2, 0, 1)), tile_count, adjacency[0, 0], messages)

    stages = bit_count(n * groups)
    halves = [
        pltpu.VMEM((pieces, half >> stage, width, lanes), jnp.bfloat16)
        for stage in range(stages)
    ]
    result = pl.pallas_call(
        functools.partial(reduce_kernel, n, groups),
        out_shape=jax.ShapeDtypeStruct((width, owned), jnp.bfloat16),
        in_specs=[whole] * 3,
        out_specs=whole,
        scratch_shapes=[pltpu.VMEM((pieces, half, width, lanes), jnp.float32)]
        + halves + halves[1:] + [
            pltpu.SemaphoreType.DMA((pieces, stages)),
            pltpu.SemaphoreType.DMA((pieces, stages)),
        ],
        compiler_params=pltpu.CompilerParams(
            collective_id=1, has_side_effects=True, vmem_limit_bytes=VMEM_LIMIT
        ),
        name="reduce",
    )(sent, kept, own)
    return result.T


def solution(mesh):
    placed = (
        P("dom", "feat"),
        P(),
        P(),
        P(),
        P(None, "dom"),
        P("dom", "feat", None, None, None),
        P("dom", "feat", None, None),
        P("dom", "feat"),
    )
    return jax.shard_map(
        functools.partial(body, mesh.shape["feat"], mesh.shape["dom"]),
        mesh=mesh, in_specs=placed, out_specs=P("dom", "feat"), check_vma=False,
    )
```
